256 devices in a mesh: occ: 8 (over z), vir: 16 (over y, x), ka: 2 (over core).
Axes of the slice: x: 4, y: 4, z: 8, core: 2. Of those that a mesh axis runs over, the one named last changes fastest.
Arguments:
- lambda_amps: bfloat16 [2, 128, 1024, 1024], P(None, 'occ', 'vir', 'ka'), may hold values from -0.25 to 0.25
- screened_ints: bfloat16 [128, 1024, 1024], P(('occ', 'vir'), 'ka'), may hold values from -6 to 6
- half_ints: bfloat16 [128, 1024, 128], P(('occ', 'vir'), 'ka'), may hold values from -0.5 to 0.5
- singles: bfloat16 [128, 1024], P(None, 'vir'), may hold values from -6 to 6
- block_mask: int32 [128, 8, 8], P('occ', 'ka'), may hold values from 0 to 1, as said below
Outputs:
- residual_part: bfloat16 [2, 128, 1024, 1024], P('ka', 'occ', 'vir')
The draws below stay inside these ranges and needn't reach their ends.
Inputs may be any that keep to these rules, and one draw needn't show every extreme that they name: `block_mask`: for each j and each of the 2 equal ranges of e blocks, between 1 and 16 of its 32 blocks are 1; some (j, range) has exactly 16.
All inputs are finite; a program needn't handle non-finite values.
Results may differ from the reference program's by a relative error of at most 0.0058.
Values may be sent and summed in bfloat16 or wider, within the bound.
A program may use at most 128 MiB of HBM per device.

```python
import jax
import jax.numpy as jnp
from jax import lax

O = 128
V = 1024
TILE = 128
CAP = 16
IW = 2
NB = 8
HALVES = 2
HT = 32
J = 128


def draw_block_mask(key, part):
    first_key, second_key, third_key = jax.random.split(key, 3)
    groups = J * HALVES
    base_draw = jax.random.randint(first_key, (groups,), 1, 6)
    counts = jnp.minimum(base_draw * base_draw, CAP)
    forced = jax.random.randint(second_key, (), 0, groups)
    counts = jnp.where(jnp.arange(groups) == forced, CAP, counts)
    scores = jax.random.randint(third_key, (groups, HT), 0, 1 << 20) * HT + jnp.arange(HT)[None, :]
    ordering = jnp.argsort(scores, axis=1, stable=True)
    ranking = jnp.argsort(ordering, axis=1, stable=True)
    live_tiles = (ranking < counts[:, None]).astype(jnp.int32)
    return live_tiles.reshape(J, NB, NB)


def levels(stream_key, shape, cuts, smallest, largest):
    def one(dim, shards_of):
        heights = jax.random.uniform(jax.random.fold_in(jax.random.fold_in(stream_key, 6), dim), (shards_of,), jnp.float32, smallest / len(cuts), largest / len(cuts))
        return jnp.repeat(jnp.exp(heights), shape[dim] // shards_of).reshape((-1,) + (1,) * (len(shape) - dim - 1))

    factor_of = one(*cuts[0])
    for cut in cuts[1:]:
        factor_of = factor_of * one(*cut)
    return factor_of


def gaussian(own_key, shape, deviation, bound, shards=(), dtype=jnp.bfloat16):
    loudness = levels(own_key, shape, shards, -0.22, 0.18) if shards else 1.0
    values = jax.random.normal(own_key, shape, jnp.float32) * deviation * loudness
    return jnp.minimum(jnp.maximum(values, -bound), bound).astype(dtype)


def setup_inputs(seed: int = 0) -> dict:
    key_list = jax.random.split(jax.random.key(seed), 6)
    return {
        "lambda_amps": gaussian(key_list[0], (IW, J, V, V), (V // 2) ** -0.5, 0.25, ((1, 8), (2, 16), (3, 2))),
        "screened_ints": gaussian(key_list[1], (J, V, V), 1.0, 6.0, ((0, 128), (1, 2))),
        "half_ints": gaussian(key_list[2], (J, V, O), O ** -0.5, 0.5, ((0, 128), (1, 2))),
        "singles": gaussian(key_list[3], (O, V), 1.0, 6.0, ((1, 16),)),
        "block_mask": draw_block_mask(jax.random.fold_in(key_list[5], 71), 0),
    }


def reference(lambda_amps, screened_ints, half_ints, singles, block_mask):
    def per_item(item):
        dressed = screened_ints[item].astype(jnp.float32) - jnp.dot(half_ints[item], singles, preferred_element_type=jnp.float32)
        block_gate = jnp.repeat(jnp.repeat(block_mask[item].astype(jnp.float32), TILE, axis=0), TILE, axis=1)
        blocks = (block_gate * dressed).astype(jnp.bfloat16)
        amp_rows = lambda_amps[:, item].reshape(IW * V, V)
        result = jnp.dot(amp_rows, blocks, preferred_element_type=jnp.float32).astype(jnp.bfloat16)
        return result.reshape(IW, V, V)

    stacked = lax.map(per_item, jnp.arange(J).astype(jnp.int32))
    return jnp.transpose(stacked, (1, 0, 2, 3))
```

```python
import functools

import jax
import jax.numpy as jnp
from jax import lax
from jax.experimental import pallas as pl
from jax.experimental.pallas import tpu as pltpu
from jax.sharding import PartitionSpec as P

MESH = pl.DeviceIdType.MESH
TILE = 128
CAP = 16
CHUNK = 4
SIDE = 4
SIGNS = (-1, 1, 1, -1)
STEPS = ((0, 0), (1, 0), (0, 1), (1, 1))


def wrap(k):
    return lax.rem(k + 2 * SIDE, SIDE)


def sign_of(k):
    return 1 - 2 * lax.rem(k, 2)


def place(x, y):
    return wrap(y) * SIDE + wrap(x)


def owner_of(x, y, q):
    sx, sy = sign_of(y), sign_of(x)
    return (place(x, y), place(x - sx, y), place(x, y - sy), place(x + sx, y + sy))[q]


def kernel(
    amps, ints, half, singles, mask, out,
    lbuf, bbuf0, bbuf1, bbuf2, bbuf3, xbuf, ybuf, tbuf, give, take, acc, done, slot, nxt,
    lsend, lrecv, lown, inload, tsend, trecv, dsend, drecv, bsend, brecv, rsend, rrecv,
    psend, precv, osend, orecv, oown,
):
    bbuf = (bbuf0, bbuf1, bbuf2, bbuf3)
    vir = lax.axis_index("vir")
    ka = lax.axis_index("ka")
    other = 1 - ka
    x, y = lax.rem(vir, SIDE), vir // SIDE
    sx, sy = sign_of(y), sign_of(x)
    peers = SIDE * SIDE

    loads = [
        pltpu.make_async_copy(
            singles.at[pl.ds(ka * 32, 32)], tbuf.at[vir // 2, lax.rem(vir, 2), ka], inload.at[0]
        ),
    ]
    loads += [
        pltpu.make_async_copy(half.at[0, pl.ds(e * TILE, TILE)], ybuf.at[e], inload.at[1 + e])
        for e in range(4)
    ]
    loads += [
        pltpu.make_async_copy(
            ints.at[0, pl.ds(e * TILE, TILE), pl.ds(b * TILE, TILE)],
            xbuf.at[b, e],
            inload.at[5 + 4 * b + e],
        )
        for b in range(8)
        for e in range(4)
    ]
    for copy in loads:
        copy.start()
    own_loads = []
    for q in range(4):
        j = owner_of(x, y, q)
        own_loads.append(pltpu.make_async_copy(amps.at[:, j], lbuf.at[q, :, 0], lown.at[q]))
    for copy in own_loads:
        copy.start()

    barrier = pltpu.get_barrier_semaphore()

    def greet(r, carry):
        pl.semaphore_signal(
            barrier, inc=1, device_id={"vir": lax.rem(vir + r, peers)}, device_id_type=MESH
        )
        return carry

    lax.fori_loop(1, peers, greet, 0)
    pl.semaphore_signal(barrier, inc=1, device_id={"ka": other}, device_id_type=MESH)

    pl.semaphore_wait(barrier, peers)

    def t_copy(r):
        return pltpu.make_async_remote_copy(
            src_ref=singles.at[pl.ds(ka * 32, 32)],
            dst_ref=tbuf.at[vir // 2, lax.rem(vir, 2), ka],
            send_sem=tsend.at[r - 1],
            recv_sem=trecv.at[r - 1],
            device_id={"vir": lax.rem(vir + r, peers)},
            device_id_type=MESH,
        )

    def t_start(r, carry):
        t_copy(r).start()
        return carry

    lax.fori_loop(1, peers, t_start, 0)

    def l_copy(q, d):
        dx, dy = STEPS[d]
        hx = wrap(x - dx * SIGNS[q] * sx * (1 - 2 * dy))
        hy = wrap(y - dy * SIGNS[q] * sy * (1 - 2 * dx))
        return pltpu.make_async_remote_copy(
            src_ref=amps.at[:, owner_of(hx, hy, q)],
            dst_ref=lbuf.at[q, :, d],
            send_sem=lsend.at[q, d - 1],
            recv_sem=lrecv.at[q, d - 1],
            device_id={"vir": place(hx, hy)},
            device_id_type=MESH,
        )

    l_copies = [[l_copy(q, d) for d in (1, 2, 3)] for q in range(4)]
    for q in range(4):
        for copy in l_copies[q]:
            copy.start()

    for q in range(4):
        j = owner_of(x, y, q)

        def count(p, c, q=q, j=j):
            live = mask[lax.shift_right_logical(p, 3), lax.bitwise_and(p, 7), j]
            slot[q, p] = live * c + (1 - live) * CAP
            return c + live

        lax.fori_loop(0, 32, count, 0)

    nxt[32] = 31

    def search(k, c):
        p = 31 - k
        live = mask[lax.shift_right_logical(p, 3), lax.bitwise_and(p, 7), vir]
        c = live * p + (1 - live) * c
        nxt[p] = c
        return c

    lax.fori_loop(0, 32, search, 31)

    for q in range(4):
        bbuf[q][CAP] = jnp.zeros((TILE, TILE), jnp.bfloat16)

    def t_wait(r, carry):
        t_copy(r).wait_recv()
        return carry

    lax.fori_loop(1, peers, t_wait, 0)
    loads[0].wait()
    d_copy = pltpu.make_async_remote_copy(
        src_ref=tbuf.at[:, :, ka],
        dst_ref=tbuf.at[:, :, ka],
        send_sem=dsend,
        recv_sem=drecv,
        device_id={"ka": other},
        device_id_type=MESH,
    )
    d_copy.start()
    d_copy.wait_recv()
    for copy in loads[1:]:
        copy.wait()

    def b_copy(axis, c):
        return pltpu.make_async_remote_copy(
            src_ref=bbuf[0].at[pl.ds(c * CHUNK, CHUNK)],
            dst_ref=bbuf[1 + axis].at[pl.ds(c * CHUNK, CHUNK)],
            send_sem=bsend.at[axis, c],
            recv_sem=brecv.at[axis, c],
            device_id={"vir": place(x, y + sy) if axis else place(x + sx, y)},
            device_id_type=MESH,
        )

    def relay_copy(axis, k):
        c = 2 * axis + k
        return pltpu.make_async_remote_copy(
            src_ref=bbuf[1 + axis].at[pl.ds(c * CHUNK, CHUNK)],
            dst_ref=bbuf[3].at[pl.ds(c * CHUNK, CHUNK)],
            send_sem=rsend.at[axis, k],
            recv_sem=rrecv.at[axis, k],
            device_id={"vir": place(x - sx, y) if axis else place(x, y - sy)},
            device_id_type=MESH,
        )

    b_copies = [[b_copy(axis, c) for c in range(4)] for axis in range(2)]
    relays = [[relay_copy(axis, k) for k in range(2)] for axis in range(2)]

    def dress(k, p):
        p = nxt[p]
        e = lax.shift_right_logical(p, 3)
        b = lax.bitwise_and(p, 7)
        inner = lax.dot_general(
            ybuf[e],
            tbuf[b].reshape(TILE, TILE),
            (((1,), (1,)), ((), ())),
            preferred_element_type=jnp.float32,
        )
        value = xbuf[b, e].astype(jnp.float32) - inner
        bbuf[0][k] = value.astype(jnp.bfloat16)
        return p + 1

    p = lax.fori_loop(0, 8, dress, 0)
    b_copies[0][0].start()
    p = lax.fori_loop(8, 12, dress, p)
    b_copies[0][1].start()
    p = lax.fori_loop(12, 16, dress, p)
    b_copies[1][2].start()
    b_copies[0][2].start()
    b_copies[1][3].start()
    b_copies[0][3].start()
    b_copies[1][0].start()
    b_copies[1][1].start()

    def give_copy(q):
        return pltpu.make_async_remote_copy(
            src_ref=give.at[q],
            dst_ref=take.at[q],
            send_sem=psend.at[q],
            recv_sem=precv.at[q],
            device_id={"ka": other},
            device_id_type=MESH,
        )

    def out_copy(q, d):
        dx, dy = STEPS[d]
        return pltpu.make_async_remote_copy(
            src_ref=done.at[q, d],
            dst_ref=out.at[0, owner_of(x, y, q)],
            send_sem=osend.at[q, d - 1],
            recv_sem=orecv.at[q, d - 1],
            device_id={"vir": place(x + dx * SIGNS[q] * sx, y + dy * SIGNS[q] * sy)},
            device_id_type=MESH,
        )

    def in_copy(q, d):
        dx, dy = STEPS[d]
        hx = wrap(x - dx * SIGNS[q] * sx * (1 - 2 * dy))
        hy = wrap(y - dy * SIGNS[q] * sy * (1 - 2 * dx))
        return pltpu.make_async_remote_copy(
            src_ref=done.at[q, d],
            dst_ref=out.at[0, owner_of(hx, hy, q)],
            send_sem=osend.at[q, d - 1],
            recv_sem=orecv.at[q, d - 1],
            device_id={"vir": place(hx, hy)},
            device_id_type=MESH,
        )

    gives = [give_copy(q) for q in range(4)]
    outs = [[out_copy(q, d) for d in (1, 2, 3)] for q in range(4)]
    own_outs = [
        pltpu.make_async_copy(done.at[q, 0], out.at[0, owner_of(x, y, q)], oown.at[q])
        for q in range(4)
    ]

    def multiply(q):
        own_loads[q].wait()
        for copy in l_copies[q]:
            copy.wait_recv()

        def columns(n, carry):
            pieces = []
            for e in range(4):
                pieces.append(
                    jnp.concatenate(
                        [bbuf[q][slot[q, 8 * e + 2 * n + k]] for k in range(2)], axis=1
                    )
                )
            rhs = jnp.concatenate(pieces, axis=0)
            where = pl.ds(pl.multiple_of(n * 2 * TILE, 2 * TILE), 2 * TILE)
            lhs = lbuf[q, other].reshape(256, 512)
            part = jnp.dot(lhs, rhs, preferred_element_type=jnp.float32)
            give[q, :, :, where] = part.astype(jnp.bfloat16).reshape(4, 64, 2 * TILE)
            lhs = lbuf[q, ka].reshape(256, 512)
            part = jnp.dot(lhs, rhs, preferred_element_type=jnp.float32)
            acc[q, :, :, where] = part.reshape(4, 64, 2 * TILE)
            return carry

        lax.fori_loop(0, 4, columns, 0)
        gives[q].start()

    def finish(q):
        gives[q].wait_recv()
        for d in (3, 1, 2, 0):
            total = acc[q, d] + take[q, d].astype(jnp.float32)
            done[q, d] = total.astype(jnp.bfloat16)
        for d in (3, 1, 2):
            outs[q][d - 1].start()
        own_outs[q].start()

    multiply(0)
    b_copies[0][0].wait_recv()
    relays[0][0].start()
    b_copies[1][2].wait_recv()
    relays[1][0].start()
    b_copies[0][1].wait_recv()
    relays[0][1].start()
    b_copies[1][3].wait_recv()
    relays[1][1].start()
    finish(0)
    b_copies[0][2].wait_recv()
    b_copies[0][3].wait_recv()
    multiply(1)
    b_copies[1][0].wait_recv()
    b_copies[1][1].wait_recv()
    multiply(2)
    finish(1)
    for axis in range(2):
        for k in range(2):
            relays[axis][k].wait_recv()
    multiply(3)
    finish(2)
    finish(3)

    def t_sent(r, carry):
        t_copy(r).wait_send()
        return carry

    lax.fori_loop(1, peers, t_sent, 0)
    d_copy.wait_send()
    for q in range(4):
        gives[q].wait_send()
        own_outs[q].wait()
        for d in (1, 2, 3):
            l_copies[q][d - 1].wait_send()
            outs[q][d - 1].wait_send()
            in_copy(q, d).wait_recv()
    for axis in range(2):
        for c in range(4):
            b_copies[axis][c].wait_send()
        for k in range(2):
            relays[axis][k].wait_send()


def body(lambda_amps, screened_ints, half_ints, singles, block_mask):
    bf16, f32 = jnp.bfloat16, jnp.float32
    dma = pltpu.SemaphoreType.DMA
    anywhere = pl.BlockSpec(memory_space=pl.ANY)
    return pl.pallas_call(
        kernel,
        out_shape=jax.ShapeDtypeStruct((1, 16, 64, 1024), bf16),
        in_specs=[anywhere] * 4 + [pl.BlockSpec(memory_space=pltpu.SMEM)],
        out_specs=anywhere,
        scratch_shapes=[
            pltpu.VMEM((4, 2, 4, 64, 512), bf16),
            pltpu.VMEM((CAP + 1, TILE, TILE), bf16),
            pltpu.VMEM((CAP + 1, TILE, TILE), bf16),
            pltpu.VMEM((CAP + 1, TILE, TILE), bf16),
            pltpu.VMEM((CAP + 1, TILE, TILE), bf16),
            pltpu.VMEM((8, 4, TILE, TILE), bf16),
            pltpu.VMEM((4, TILE, TILE), bf16),
            pltpu.VMEM((8, 2, 2, 32, TILE), bf16),
            pltpu.VMEM((4, 4, 64, 1024), bf16),
            pltpu.VMEM((4, 4, 64, 1024), bf16),
            pltpu.VMEM((4, 4, 64, 1024), f32),
            pltpu.VMEM((4, 4, 64, 1024), bf16),
            pltpu.SMEM((4, 32), jnp.int32),
            pltpu.SMEM((40,), jnp.int32),
            dma((4, 3)), dma((4, 3)), dma((4,)), dma((37,)),
            dma((15,)), dma((15,)), dma, dma,
            dma((2, 4)), dma((2, 4)), dma((2, 2)), dma((2, 2)),
            dma((4,)), dma((4,)), dma((4, 3)), dma((4, 3)), dma((4,)),
        ],
        compiler_params=pltpu.CompilerParams(collective_id=0, has_side_effects=True),
        cost_estimate=pl.CostEstimate(
            flops=2 * 2048 * 512 * 1024, bytes_accessed=6 << 20, transcendentals=0
        ),
    )(lambda_amps, screened_ints, half_ints, singles.T, jnp.transpose(block_mask, (1, 2, 0)))


def solution(mesh):
    return jax.shard_map(
        body,
        mesh=mesh,
        in_specs=(
            P(None, "occ", "vir", "ka"),
            P(("occ", "vir"), "ka", None),
            P(("occ", "vir"), "ka", None),
            P(None, "vir"),
            P("occ", "ka", None),
        ),
        out_specs=P("ka", "occ", "vir", None),
        check_vma=False,
    )
```

```python
import jax
import jax.numpy as jnp
from jax import lax
from jax.experimental import pallas as pl
from jax.experimental.pallas import tpu as pltpu
from jax.sharding import PartitionSpec as P

MESH = pl.DeviceIdType.MESH
TILE = 128
CHUNK = 5
EMPTY = 20
SIDE = 4
HOLD = ((0, 0), (1, 0), (0, 1), (1, 1))
AROUND = tuple((a, b) for a in (-1, 0, 1) for b in (-1, 0, 1) if (a, b) != (0, 0))
EDGES = (
    (0, 1, (1, 0), (0, 2, 3)),
    (0, 2, (0, 1), (1, 2, 3)),
    (1, 3, (0, 1), (0, 2)),
    (2, 3, (1, 0), (1, 3)),
    (3, 2, (-1, 0), (0,)),
    (3, 1, (0, -1), (1,)),
)
START = (
    (1, 1, 0), (1, 2, 1), (0, 0, 1), (0, 0, 2), (1, 1, 2), (1, 2, 2), (0, 1, 1), (0, 2, 2),
    (1, 1, 3), (1, 2, 3),
)
MIDDLE = ((0, 3), (1, 3), (2, 3), (1, 2), (2, 1))
LATE = ((3, 3), (3, 1), (3, 2))
RELAYS = (
    ((1, -1), (-1, 0)), ((1, 0), (-1, 0)), ((1, 1), (-1, 0)),
    ((-1, 1), (0, -1)), ((0, 1), (0, -1)), ((1, 1), (0, -1)),
    ((1, 1), (-1, -1)),
)


def served(q):
    ax, ay = HOLD[q]
    ux, uy = 2 * ax - 1, 2 * ay - 1
    return ((0, 0), (ux, 0), (0, uy), (ux, uy))


def parity(a, b):
    return 1 - 2 * ((a + b) % 2)


def wrap(k):
    return lax.rem(k + 2 * SIDE, SIDE)


def place(x, y):
    return wrap(y) * SIDE + wrap(x)


def kernel(
    amps, ints, half, singles, mask_in, out,
    lbuf, bbuf0, bbuf1, bbuf2, bbuf3, xbuf, tbuf, give, take, acc, done,
    mask, slot, nxt,
    lsend, lrecv, lown, inload, tsend, trecv, rsend, rrecv, dsend, drecv, bsend, brecv,
    psend, precv, osend, orecv,
):
    bbuf = (bbuf0, bbuf1, bbuf2, bbuf3)
    vir = lax.axis_index("vir")
    ka = lax.axis_index("ka")
    other = 1 - ka
    x, y = lax.rem(vir, SIDE), vir // SIDE
    sign = 1 - 2 * lax.rem(x + y, 2)

    def near(a, b):
        return place(x + a, y + b)

    def block(v):
        return tbuf.at[v // 2, lax.rem(v, 2), ka]

    def held(q):
        ax, ay = HOLD[q]
        s = sign * parity(ax, ay)
        return near(-s * ax, -s * ay)

    def remote(src, dst, send, recv, v):
        return pltpu.make_async_remote_copy(
            src_ref=src, dst_ref=dst, send_sem=send, recv_sem=recv,
            device_id={"vir": v}, device_id_type=MESH,
        )

    def partner(src, dst, send, recv):
        return pltpu.make_async_remote_copy(
            src_ref=src, dst_ref=dst, send_sem=send, recv_sem=recv,
            device_id={"ka": other}, device_id_type=MESH,
        )

    barrier = pltpu.get_barrier_semaphore()
    for a, b in AROUND:
        pl.semaphore_signal(
            barrier, inc=1, device_id={"vir": near(a, b)}, device_id_type=MESH
        )
    pl.semaphore_signal(barrier, inc=1, device_id={"ka": other}, device_id_type=MESH)

    own_t = pltpu.make_async_copy(singles.at[pl.ds(ka * 32, 32)], block(vir), inload.at[0])
    own_t.start()
    mask_load = pltpu.make_async_copy(mask_in, mask, inload.at[1])
    mask_load.start()
    loads = [
        pltpu.make_async_copy(half.at[0, pl.ds(e * TILE, TILE)], bbuf0.at[CHUNK * e + 4], inload.at[2 + e])
        for e in range(4)
    ]
    loads += [
        pltpu.make_async_copy(
            ints.at[0, pl.ds(e * TILE, TILE), pl.ds(b * TILE, TILE)],
            xbuf.at[b, e],
            inload.at[6 + 4 * b + e],
        )
        for b in range(8)
        for e in range(4)
    ]
    loads += [
        pltpu.make_async_copy(amps.at[:, held(q)], lbuf.at[q, :, 0], lown.at[q])
        for q in range(4)
    ]
    for copy in loads:
        copy.start()
    own_l = loads[-4:]
    loads = loads[:-4]

    t_first = [
        remote(block(vir), block(vir), tsend.at[k], trecv.at[k], near(a, b))
        for k, (a, b) in enumerate(AROUND)
    ]
    t_from = [
        remote(block(near(-a, -b)), block(near(-a, -b)), tsend.at[k], trecv.at[k], near(a, b))
        for k, (a, b) in enumerate(AROUND)
    ]
    t_second = [
        remote(block(near(*what)), block(near(*what)), rsend.at[k], rrecv.at[k], near(*to))
        for k, (what, to) in enumerate(RELAYS)
    ]
    t_second_from = [
        remote(
            block(near(what[0] - to[0], what[1] - to[1])),
            block(near(what[0] - to[0], what[1] - to[1])),
            rsend.at[k], rrecv.at[k], near(*to),
        )
        for k, (what, to) in enumerate(RELAYS)
    ]

    def holder(q, d):
        ax, ay = HOLD[q]
        dx, dy = served(q)[d]
        s = sign * parity(ax + dx, ay + dy)
        return near(-s * dx, -s * dy), near(-s * (ax + dx), -s * (ay + dy))

    l_copies, ins = {}, {}
    for q in range(4):
        for d in (1, 2, 3):
            h, j = holder(q, d)
            l_copies[q, d] = remote(
                amps.at[:, j], lbuf.at[q, :, d], lsend.at[q, d - 1], lrecv.at[q, d - 1], h
            )
            ins[q, d] = remote(
                done.at[q, d - 1], out.at[0, j], osend.at[q, d - 1], orecv.at[q, d - 1], h
            )

    b_copies = {}
    for p, q, (dx, dy), chunks in EDGES:
        s = sign * parity(*HOLD[p])
        for c in chunks:
            piece = pl.ds(c * CHUNK, CHUNK)
            b_copies[q, c] = remote(
                bbuf[p].at[piece], bbuf[q].at[piece],
                bsend.at[q - 1, c], brecv.at[q - 1, c], near(s * dx, s * dy),
            )

    gives = [partner(give.at[q], take.at[q], psend.at[q], precv.at[q]) for q in range(4)]

    outs = {}
    for q in range(4):
        s = sign * parity(*HOLD[q])
        for d in (1, 2, 3):
            dx, dy = served(q)[d]
            outs[q, d] = remote(
                done.at[q, d - 1], out.at[0, held(q)],
                osend.at[q, d - 1], orecv.at[q, d - 1], near(s * dx, s * dy),
            )

    mask_load.wait()
    for q in range(4):
        j = held(q)

        def count(p, c, q=q, j=j):
            live = mask[lax.shift_right_logical(p, 3), lax.bitwise_and(p, 7), j]
            slot[q, p] = live * (c + lax.shift_right_logical(c, 2)) + (1 - live) * EMPTY
            return c + live

        lax.fori_loop(0, 32, count, 0)
        bbuf[q][EMPTY] = jnp.zeros((TILE, TILE), jnp.bfloat16)

    nxt[32] = 31

    def search(k, c):
        p = 31 - k
        live = mask[lax.shift_right_logical(p, 3), lax.bitwise_and(p, 7), vir]
        c = live * p + (1 - live) * c
        nxt[p] = c
        return c

    lax.fori_loop(0, 32, search, 31)

    for copy in loads:
        copy.wait()

    def pack(k, p):
        p = nxt[p]
        bbuf0[k + lax.shift_right_logical(k, 2)] = xbuf[
            lax.bitwise_and(p, 7), lax.shift_right_logical(p, 3)
        ]
        return p + 1

    lax.fori_loop(0, 16, pack, 0)

    own_t.wait()
    pl.semaphore_wait(barrier, 9)

    for copy in t_first:
        copy.start()
    for kind, one, two in START:
        (b_copies if kind else l_copies)[one, two].start()
    for copy in t_from:
        copy.wait_recv()
    for copy in t_second:
        copy.start()

    def multiply(q):
        own_l[q].wait()
        for d in (1, 2, 3):
            l_copies[q, d].wait_recv()
        j = held(q)

        def columns(n, carry):
            amount = jnp.concatenate([bbuf[q][CHUNK * e + 4] for e in range(4)], axis=0)
            inner = lax.dot_general(
                amount,
                tbuf[pl.ds(2 * n, 2)].reshape(2 * TILE, TILE),
                (((1,), (1,)), ((), ())),
                preferred_element_type=jnp.float32,
            )
            pieces = []
            for e in range(4):
                row = []
                for k in range(2):
                    gate = mask[e, 2 * n + k, j].astype(jnp.float32)
                    value = bbuf[q][slot[q, 8 * e + 2 * n + k]].astype(jnp.float32)
                    value -= inner[e * TILE : (e + 1) * TILE, k * TILE : (k + 1) * TILE]
                    row.append((gate * value).astype(jnp.bfloat16))
                pieces.append(jnp.concatenate(row, axis=1))
            rhs = jnp.concatenate(pieces, axis=0)
            where = pl.ds(pl.multiple_of(n * 2 * TILE, 2 * TILE), 2 * TILE)
            lhs = lbuf[q, other].reshape(256, 512)
            part = jnp.dot(lhs, rhs, preferred_element_type=jnp.float32)
            give[q, :, :, where] = part.astype(jnp.bfloat16).reshape(4, 64, 2 * TILE)
            lhs = lbuf[q, ka].reshape(256, 512)
            part = jnp.dot(lhs, rhs, preferred_element_type=jnp.float32)
            acc[q, :, :, where] = part.reshape(4, 64, 2 * TILE)
            return carry

        lax.fori_loop(0, 4, columns, 0)
        gives[q].start()

    def finish(q, ds):
        for d in ds:
            total = acc[q, d] + take[q, d].astype(jnp.float32)
            if d:
                done[q, d - 1] = total.astype(jnp.bfloat16)
            else:
                out[0, held(q)] = total.astype(jnp.bfloat16)

    def send(*which):
        for q, d in which:
            outs[q, d].start()

    def relay(q, c, r):
        b_copies[q, c].wait_recv()
        b_copies[r, c].start()

    relay(1, 0, 3)
    relay(2, 1, 3)
    for q, d in MIDDLE:
        l_copies[q, d].start()
    relay(1, 2, 3)
    relay(3, 0, 2)
    relay(3, 1, 1)
    relay(2, 3, 3)
    for q, d in LATE:
        l_copies[q, d].start()

    for copy in t_second_from:
        copy.wait_recv()
    t_half = partner(tbuf.at[:, :, ka], tbuf.at[:, :, ka], dsend, drecv)
    t_half.start()
    partner(tbuf.at[:, :, other], tbuf.at[:, :, other], dsend, drecv).wait_recv()

    multiply(0)
    gives[0].wait_recv()
    finish(0, (0, 1, 2, 3))
    send((0, 3), (0, 1), (0, 2))
    for c in (1, 3):
        b_copies[1, c].wait_recv()
    multiply(1)
    for c in (0, 2):
        b_copies[2, c].wait_recv()
    multiply(2)
    gives[1].wait_recv()
    finish(1, (3, 1, 2, 0))
    gives[2].wait_recv()
    finish(2, (3, 1, 2, 0))
    send((1, 3), (2, 3), (1, 1), (2, 1), (1, 2), (2, 2))
    for c in (2, 3):
        b_copies[3, c].wait_recv()
    multiply(3)
    gives[3].wait_recv()
    finish(3, (3, 1, 2, 0))
    send((3, 3), (3, 1), (3, 2))

    for copy in t_first + t_second + [t_half] + gives:
        copy.wait_send()
    for copies in (l_copies, b_copies, outs):
        for copy in copies.values():
            copy.wait_send()
    for copy in ins.values():
        copy.wait_recv()


def body(lambda_amps, screened_ints, half_ints, singles, block_mask):
    bf16, f32 = jnp.bfloat16, jnp.float32
    dma = pltpu.SemaphoreType.DMA
    anywhere = pl.BlockSpec(memory_space=pl.ANY)
    return pl.pallas_call(
        kernel,
        out_shape=pltpu.VMEM((1, 16, 64, 1024), bf16),
        in_specs=[anywhere] * 5,
        out_specs=pl.BlockSpec(memory_space=pltpu.VMEM),
        scratch_shapes=[
            pltpu.VMEM((4, 2, 4, 64, 512), bf16),
            pltpu.VMEM((EMPTY + 1, TILE, TILE), bf16),
            pltpu.VMEM((EMPTY + 1, TILE, TILE), bf16),
            pltpu.VMEM((EMPTY + 1, TILE, TILE), bf16),
            pltpu.VMEM((EMPTY + 1, TILE, TILE), bf16),
            pltpu.VMEM((8, 4, TILE, TILE), bf16),
            pltpu.VMEM((8, 2, 2, 32, TILE), bf16),
            pltpu.VMEM((4, 4, 64, 1024), bf16),
            pltpu.VMEM((4, 4, 64, 1024), bf16),
            pltpu.VMEM((4, 4, 64, 1024), f32),
            pltpu.VMEM((4, 3, 64, 1024), bf16),
            pltpu.SMEM((4, 8, 16), jnp.int32),
            pltpu.SMEM((4, 32), jnp.int32),
            pltpu.SMEM((40,), jnp.int32),
            dma((4, 3)), dma((4, 3)), dma((4,)), dma((38,)),
            dma((8,)), dma((8,)), dma((7,)), dma((7,)), dma, dma,
            dma((3, 4)), dma((3, 4)),
            dma((4,)), dma((4,)), dma((4, 3)), dma((4, 3)),
        ],
        compiler_params=pltpu.CompilerParams(collective_id=0, has_side_effects=True),
        cost_estimate=pl.CostEstimate(
            flops=2 * 2048 * 512 * 1024, bytes_accessed=6 << 20, transcendentals=0
        ),
    )(
        lambda_amps, screened_ints, half_ints, singles.T,
        jnp.transpose(block_mask, (1, 2, 0)),
    )


def solution(mesh):
    return jax.shard_map(
        body,
        mesh=mesh,
        in_specs=(
            P(None, "occ", "vir", "ka"),
            P(("occ", "vir"), "ka", None),
            P(("occ", "vir"), "ka", None),
            P(None, "vir"),
            P("occ", "ka", None),
        ),
        out_specs=P("ka", "occ", "vir", None),
        check_vma=False,
    )
```

```python
import jax
import jax.numpy as jnp
from jax import lax
from jax.experimental import pallas as pl
from jax.experimental.pallas import tpu as pltpu
from jax.sharding import PartitionSpec as P

MESH = pl.DeviceIdType.MESH
TILE = 128
CHUNK = 5
EMPTY = 20
LAG = 5
SIDE = 4
HOLD = ((0, 0), (1, 0), (0, 1), (1, 1))
AROUND = tuple((a, b) for a in (-1, 0, 1) for b in (-1, 0, 1) if (a, b) != (0, 0))
EDGES = (
    (0, 1, (1, 0), (0, 1, 4, 5, 6, 7)),
    (0, 2, (0, 1), (2, 3, 4, 5, 6, 7)),
    (1, 3, (0, 1), (0, 1, 4, 5)),
    (2, 3, (1, 0), (2, 3, 6, 7)),
    (3, 2, (-1, 0), (0, 1)),
    (3, 1, (0, -1), (2, 3)),
)
PIECES = tuple((CHUNK * (c // 2) + 3 * (c % 2), 3 - c % 2) for c in range(8))
RELAYS = (
    ((1, -1), (-1, 0)), ((1, 0), (-1, 0)), ((1, 1), (-1, 0)),
    ((-1, 1), (0, -1)), ((0, 1), (0, -1)), ((1, 1), (0, -1)),
    ((1, 1), (-1, -1)),
)


def served(q):
    ax, ay = HOLD[q]
    ux, uy = 2 * ax - 1, 2 * ay - 1
    return ((0, 0), (ux, 0), (0, uy), (ux, uy))


def parity(a, b):
    return 1 - 2 * ((a + b) % 2)


def wrap(k):
    return lax.rem(k + 2 * SIDE, SIDE)


def place(x, y):
    return wrap(y) * SIDE + wrap(x)


def kernel(
    amps, ints, half, singles, mask_in, out,
    lbuf, bbuf0, bbuf1, bbuf2, bbuf3, xbuf, tbuf, dense, give, take, acc, done,
    mask, slot, nxt,
    lsend, lrecv, lown, inload, tsend, trecv, rsend, rrecv, dsend, drecv, bsend, brecv,
    psend, precv, osend, orecv,
):
    bbuf = (bbuf0, bbuf1, bbuf2, bbuf3)
    vir = lax.axis_index("vir")
    ka = lax.axis_index("ka")
    other = 1 - ka
    x, y = lax.rem(vir, SIDE), vir // SIDE
    sign = 1 - 2 * lax.rem(x + y, 2)

    def near(a, b):
        return place(x + a, y + b)

    def block(v):
        return tbuf.at[v // 2, lax.rem(v, 2), ka]

    def held(q):
        ax, ay = HOLD[q]
        s = sign * parity(ax, ay)
        return near(-s * ax, -s * ay)

    def remote(src, dst, send, recv, v):
        return pltpu.make_async_remote_copy(
            src_ref=src, dst_ref=dst, send_sem=send, recv_sem=recv,
            device_id={"vir": v}, device_id_type=MESH,
        )

    def partner(src, dst, send, recv):
        return pltpu.make_async_remote_copy(
            src_ref=src, dst_ref=dst, send_sem=send, recv_sem=recv,
            device_id={"ka": other}, device_id_type=MESH,
        )

    barrier = pltpu.get_barrier_semaphore()
    for a, b in AROUND:
        pl.semaphore_signal(
            barrier, inc=1, device_id={"vir": near(a, b)}, device_id_type=MESH
        )
    pl.semaphore_signal(barrier, inc=1, device_id={"ka": other}, device_id_type=MESH)

    own_t = pltpu.make_async_copy(singles.at[pl.ds(ka * 32, 32)], block(vir), inload.at[0])
    own_t.start()
    mask_load = pltpu.make_async_copy(mask_in, mask, inload.at[1])
    mask_load.start()
    loads = [
        pltpu.make_async_copy(half.at[0, pl.ds(e * TILE, TILE)], bbuf0.at[CHUNK * e + 4], inload.at[2 + e])
        for e in range(4)
    ]
    loads += [
        pltpu.make_async_copy(
            ints.at[0, pl.ds(e * TILE, TILE), pl.ds(b * TILE, TILE)],
            xbuf.at[b, e],
            inload.at[6 + 4 * b + e],
        )
        for b in range(8)
        for e in range(4)
    ]
    loads += [
        pltpu.make_async_copy(amps.at[:, held(q)], lbuf.at[q, :, 0], lown.at[q])
        for q in range(4)
    ]
    for copy in loads:
        copy.start()
    own_l = loads[-4:]
    loads = loads[:-4]

    t_first = [
        remote(block(vir), block(vir), tsend.at[k], trecv.at[k], near(a, b))
        for k, (a, b) in enumerate(AROUND)
    ]
    t_from = [
        remote(block(near(-a, -b)), block(near(-a, -b)), tsend.at[k], trecv.at[k], near(a, b))
        for k, (a, b) in enumerate(AROUND)
    ]
    t_second, t_second_from = [], []
    for k, ((a, b), (to_x, to_y)) in enumerate(RELAYS):
        what = block(near(sign * a, sign * b))
        to = near(sign * to_x, sign * to_y)
        t_second.append(remote(what, what, rsend.at[k], rrecv.at[k], to))
        s = sign * parity(to_x, to_y)
        what = block(near(s * (a - to_x), s * (b - to_y)))
        t_second_from.append(remote(what, what, rsend.at[k], rrecv.at[k], to))

    def holder(q, d):
        ax, ay = HOLD[q]
        dx, dy = served(q)[d]
        s = sign * parity(ax + dx, ay + dy)
        return near(-s * dx, -s * dy), near(-s * (ax + dx), -s * (ay + dy))

    l_copies, ins = {}, {}
    for q in range(4):
        for d in (1, 2, 3):
            h, j = holder(q, d)
            l_copies[q, d] = remote(
                amps.at[:, j], lbuf.at[q, :, d], lsend.at[q, d - 1], lrecv.at[q, d - 1], h
            )
            ins[q, d] = remote(
                done.at[q, d - 1], out.at[0, j], osend.at[q, d - 1], orecv.at[q, d - 1], h
            )

    b_copies = {}
    for p, q, (dx, dy), chunks in EDGES:
        s = sign * parity(*HOLD[p])
        for c in chunks:
            piece = pl.ds(*PIECES[c])
            b_copies[q, c] = remote(
                bbuf[p].at[piece], bbuf[q].at[piece],
                bsend.at[q - 1, c], brecv.at[q - 1, c], near(s * dx, s * dy),
            )

    gives = {}
    for q in range(4):
        for d in range(4):
            gives[q, d] = partner(
                give.at[q, d], take.at[q, d], psend.at[q, d], precv.at[q, d]
            )

    outs = {}
    for q in range(4):
        s = sign * parity(*HOLD[q])
        for d in (1, 2, 3):
            dx, dy = served(q)[d]
            outs[q, d] = remote(
                done.at[q, d - 1], out.at[0, held(q)],
                osend.at[q, d - 1], orecv.at[q, d - 1], near(s * dx, s * dy),
            )

    mask_load.wait()
    nxt[32] = 31

    def search(k, c):
        p = 31 - k
        live = mask[lax.shift_right_logical(p, 3), lax.bitwise_and(p, 7), vir]
        c = live * p + (1 - live) * c
        nxt[p] = c
        return c

    lax.fori_loop(0, 32, search, 31)

    for copy in loads:
        copy.wait()

    def pack(k, p):
        p = nxt[p]
        bbuf0[k + lax.shift_right_logical(k, 2)] = xbuf[
            lax.bitwise_and(p, 7), lax.shift_right_logical(p, 3)
        ]
        return p + 1

    lax.fori_loop(0, 16, pack, 0)

    def dress(q):
        j = held(q)

        def columns(n, carry):
            amount = jnp.concatenate([bbuf[q][CHUNK * e + 4] for e in range(4)], axis=0)
            inner = lax.dot_general(
                amount,
                tbuf[pl.ds(2 * n, 2)].reshape(2 * TILE, TILE),
                (((1,), (1,)), ((), ())),
                preferred_element_type=jnp.float32,
            )
            for e in range(4):
                for k in range(2):
                    gate = mask[e, 2 * n + k, j].astype(jnp.float32)
                    value = bbuf[q][slot[q, 8 * e + 2 * n + k]].astype(jnp.float32)
                    value -= inner[e * TILE : (e + 1) * TILE, k * TILE : (k + 1) * TILE]
                    dense[q, n, e * TILE : (e + 1) * TILE, k * TILE : (k + 1) * TILE] = (
                        gate * value
                    ).astype(jnp.bfloat16)
            return carry

        lax.fori_loop(0, 4, columns, 0)

    def multiply(q, d):
        if d:
            l_copies[q, d].wait_recv()
        else:
            own_l[q].wait()
        lhs = jnp.concatenate([lbuf[q, other, d], lbuf[q, ka, d]], axis=0)
        for n in range(4):
            where = pl.ds(n * 2 * TILE, 2 * TILE)
            part = jnp.dot(lhs, dense[q, n], preferred_element_type=jnp.float32)
            give[q, d, :, where] = part[:64].astype(jnp.bfloat16)
            acc[q, d, :, where] = part[64:]
        gives[q, d].start()

    def finish(q, d):
        gives[q, d].wait_recv()
        total = acc[q, d] + take[q, d].astype(jnp.float32)
        if d:
            done[q, d - 1] = total.astype(jnp.bfloat16)
            outs[q, d].start()
        else:
            out[0, held(q)] = total.astype(jnp.bfloat16)

    def tables():
        for q in range(4):
            j = held(q)

            def count(p, c, q=q, j=j):
                live = mask[lax.shift_right_logical(p, 3), lax.bitwise_and(p, 7), j]
                slot[q, p] = live * (c + lax.shift_right_logical(c, 2)) + (1 - live) * EMPTY
                return c + live

            lax.fori_loop(0, 32, count, 0)
            bbuf[q][EMPTY] = jnp.zeros((TILE, TILE), jnp.bfloat16)

    def units(*which):
        for k, unit in enumerate(which):
            multiply(*unit)
            if k >= LAG:
                finish(*which[k - LAG])
        for unit in which[-LAG:]:
            finish(*unit)

    def rows(*which):
        for q, d in which:
            l_copies[q, d].start()

    def blocks(q, *which):
        for c in which:
            b_copies[q, c].start()

    def arrived(q, *which):
        for c in which:
            b_copies[q, c].wait_recv()

    t_half = partner(tbuf.at[:, :, ka], tbuf.at[:, :, ka], dsend, drecv)
    t_other = partner(tbuf.at[:, :, other], tbuf.at[:, :, other], dsend, drecv)

    def t_on():
        for copy in t_from:
            copy.wait_recv()
        for copy in t_second:
            copy.start()

    def t_across():
        for copy in t_second_from:
            copy.wait_recv()
        t_half.start()

    def relay(q, c, r):
        b_copies[q, c].wait_recv()
        b_copies[r, c].start()

    own_t.wait()
    pl.semaphore_wait(barrier, 9)

    for copy in t_first:
        copy.start()
    blocks(1, 0, 1)
    blocks(2, 2, 3)
    rows((0, 1), (0, 2))
    blocks(1, 4, 5)
    blocks(2, 4, 5)
    blocks(1, 6, 7)
    blocks(2, 6, 7)
    rows((3, 1), (3, 2), (2, 1), (1, 2))
    tables()
    relay(1, 0, 3)
    relay(2, 2, 3)
    t_on()
    relay(1, 1, 3)
    relay(2, 3, 3)
    relay(3, 0, 2)
    relay(3, 2, 1)
    t_across()
    relay(3, 1, 2)
    relay(3, 3, 1)
    relay(1, 4, 3)
    relay(1, 5, 3)
    relay(2, 6, 3)
    relay(2, 7, 3)
    rows((1, 3), (1, 1), (2, 2), (0, 3), (3, 3), (2, 3))
    t_other.wait_recv()
    dress(0)
    multiply(0, 1)
    multiply(0, 2)
    multiply(0, 0)
    arrived(2, 0, 1, 4, 5)
    dress(2)
    finish(0, 1)
    finish(0, 2)
    multiply(2, 1)
    arrived(3, 4, 5, 6, 7)
    dress(3)
    multiply(3, 1)
    multiply(3, 2)
    finish(2, 1)
    arrived(1, 2, 3, 6, 7)
    dress(1)
    multiply(1, 2)
    multiply(1, 1)
    finish(3, 1)
    finish(3, 2)
    multiply(1, 3)
    multiply(1, 0)
    multiply(2, 0)
    finish(1, 2)
    finish(1, 1)
    multiply(2, 2)
    multiply(3, 0)
    finish(1, 3)
    multiply(0, 3)
    finish(2, 2)
    multiply(3, 3)
    multiply(2, 3)
    finish(0, 3)
    finish(3, 3)
    finish(2, 3)
    finish(0, 0)
    finish(1, 0)
    finish(2, 0)
    finish(3, 0)

    for copy in t_first + t_second + [t_half]:
        copy.wait_send()
    for copies in (l_copies, b_copies, outs, gives):
        for copy in copies.values():
            copy.wait_send()
    for copy in ins.values():
        copy.wait_recv()

def body(lambda_amps, screened_ints, half_ints, singles, block_mask):
    bf16, f32 = jnp.bfloat16, jnp.float32
    dma = pltpu.SemaphoreType.DMA
    anywhere = pl.BlockSpec(memory_space=pl.ANY)
    return pl.pallas_call(
        kernel,
        out_shape=pltpu.VMEM((1, 16, 64, 1024), bf16),
        in_specs=[anywhere] * 5,
        out_specs=pl.BlockSpec(memory_space=pltpu.VMEM),
        scratch_shapes=[
            pltpu.VMEM((4, 2, 4, 64, 512), bf16),
            pltpu.VMEM((EMPTY + 1, TILE, TILE), bf16),
            pltpu.VMEM((EMPTY + 1, TILE, TILE), bf16),
            pltpu.VMEM((EMPTY + 1, TILE, TILE), bf16),
            pltpu.VMEM((EMPTY + 1, TILE, TILE), bf16),
            pltpu.VMEM((8, 4, TILE, TILE), bf16),
            pltpu.VMEM((8, 2, 2, 32, TILE), bf16),
            pltpu.VMEM((4, 4, 512, 2 * TILE), bf16),
            pltpu.VMEM((4, 4, 64, 1024), bf16),
            pltpu.VMEM((4, 4, 64, 1024), bf16),
            pltpu.VMEM((4, 4, 64, 1024), f32),
            pltpu.VMEM((4, 3, 64, 1024), bf16),
            pltpu.SMEM((4, 8, 16), jnp.int32),
            pltpu.SMEM((4, 32), jnp.int32),
            pltpu.SMEM((40,), jnp.int32),
            dma((4, 3)), dma((4, 3)), dma((4,)), dma((38,)),
            dma((8,)), dma((8,)), dma((7,)), dma((7,)), dma, dma,
            dma((3, 8)), dma((3, 8)),
            dma((4, 4)), dma((4, 4)), dma((4, 3)), dma((4, 3)),
        ],
        compiler_params=pltpu.CompilerParams(collective_id=0, has_side_effects=True),
        cost_estimate=pl.CostEstimate(
            flops=2 * 2048 * 512 * 1024, bytes_accessed=6 << 20, transcendentals=0
        ),
    )(
        lambda_amps, screened_ints, half_ints, singles.T,
        jnp.transpose(block_mask, (1, 2, 0)),
    )


def solution(mesh):
    return jax.shard_map(
        body,
        mesh=mesh,
        in_specs=(
            P(None, "occ", "vir", "ka"),
            P(("occ", "vir"), "ka", None),
            P(("occ", "vir"), "ka", None),
            P(None, "vir"),
            P("occ", "ka", None),
        ),
        out_specs=P("ka", "occ", "vir", None),
        check_vma=False,
    )
```

```python
import jax
import jax.numpy as jnp
from jax import lax
from jax.experimental import pallas as pl
from jax.experimental.pallas import tpu as pltpu
from jax.sharding import PartitionSpec as P

MESH = pl.DeviceIdType.MESH
TILE = 128
CHUNK = 5
EMPTY = 20
LAG = 5
SIDE = 4
HOLD = ((0, 0), (1, 0), (0, 1), (1, 1))
AROUND = tuple((a, b) for a in (-1, 0, 1) for b in (-1, 0, 1) if (a, b) != (0, 0))
EDGES = (
    (0, 1, (1, 0), (0, 1, 4, 5, 6, 7)),
    (0, 2, (0, 1), (2, 3, 4, 5, 6, 7)),
    (1, 3, (0, 1), (0, 1, 4, 5)),
    (2, 3, (1, 0), (2, 3, 6, 7)),
    (3, 2, (-1, 0), (0, 1)),
    (3, 1, (0, -1), (2, 3)),
)
PIECES = tuple((CHUNK * (c // 2) + 3 * (c % 2), 3 - c % 2) for c in range(8))
RELAYS = (
    ((1, -1), (-1, 0)), ((1, 0), (-1, 0)), ((1, 1), (-1, 0)),
    ((-1, 1), (0, -1)), ((0, 1), (0, -1)), ((1, 1), (0, -1)),
    ((1, 1), (-1, -1)),
)


def served(q):
    ax, ay = HOLD[q]
    ux, uy = 2 * ax - 1, 2 * ay - 1
    return ((0, 0), (ux, 0), (0, uy), (ux, uy))


def parity(a, b):
    return 1 - 2 * ((a + b) % 2)


def wrap(k):
    return lax.rem(k + 2 * SIDE, SIDE)


def place(x, y):
    return wrap(y) * SIDE + wrap(x)


def kernel(
    amps, ints, half, singles, mask_in, out,
    lbuf, bbuf0, bbuf1, bbuf2, bbuf3, xbuf, tbuf, dense, give, take, acc, done,
    mask, slot, nxt,
    lsend, lrecv, lown, inload, tsend, trecv, rsend, rrecv, dsend, drecv, bsend, brecv,
    psend, precv, osend, orecv,
):
    bbuf = (bbuf0, bbuf1, bbuf2, bbuf3)
    vir = lax.axis_index("vir")
    ka = lax.axis_index("ka")
    other = 1 - ka
    x, y = lax.rem(vir, SIDE), vir // SIDE
    sign = 1 - 2 * lax.rem(x + y, 2)

    def near(a, b):
        return place(x + a, y + b)

    def block(v):
        return tbuf.at[v // 2, lax.rem(v, 2), ka]

    def held(q):
        ax, ay = HOLD[q]
        s = sign * parity(ax, ay)
        return near(-s * ax, -s * ay)

    def remote(src, dst, send, recv, v):
        return pltpu.make_async_remote_copy(
            src_ref=src, dst_ref=dst, send_sem=send, recv_sem=recv,
            device_id={"vir": v}, device_id_type=MESH,
        )

    def partner(src, dst, send, recv):
        return pltpu.make_async_remote_copy(
            src_ref=src, dst_ref=dst, send_sem=send, recv_sem=recv,
            device_id={"ka": other}, device_id_type=MESH,
        )

    barrier = pltpu.get_barrier_semaphore()
    for a, b in AROUND:
        pl.semaphore_signal(
            barrier, inc=1, device_id={"vir": near(a, b)}, device_id_type=MESH
        )
    pl.semaphore_signal(barrier, inc=1, device_id={"ka": other}, device_id_type=MESH)

    own_t = pltpu.make_async_copy(singles.at[pl.ds(ka * 32, 32)], block(vir), inload.at[0])
    own_t.start()
    mask_load = pltpu.make_async_copy(mask_in, mask, inload.at[1])
    mask_load.start()
    loads = [
        pltpu.make_async_copy(half.at[0, pl.ds(e * TILE, TILE)], bbuf0.at[CHUNK * e + 4], inload.at[2 + e])
        for e in range(4)
    ]
    loads += [
        pltpu.make_async_copy(
            ints.at[0, pl.ds(e * TILE, TILE), pl.ds(b * TILE, TILE)],
            xbuf.at[b, e],
            inload.at[6 + 4 * b + e],
        )
        for b in range(8)
        for e in range(4)
    ]
    loads += [
        pltpu.make_async_copy(amps.at[:, held(q)], lbuf.at[q, :, 0], lown.at[q])
        for q in range(4)
    ]
    for copy in loads:
        copy.start()
    own_l = loads[-4:]
    loads = loads[:-4]

    t_first = [
        remote(block(vir), block(vir), tsend.at[k], trecv.at[k], near(a, b))
        for k, (a, b) in enumerate(AROUND)
    ]
    t_from = [
        remote(block(near(-a, -b)), block(near(-a, -b)), tsend.at[k], trecv.at[k], near(a, b))
        for k, (a, b) in enumerate(AROUND)
    ]
    t_second, t_second_from = [], []
    for k, ((a, b), (to_x, to_y)) in enumerate(RELAYS):
        what = block(near(sign * a, sign * b))
        to = near(sign * to_x, sign * to_y)
        t_second.append(remote(what, what, rsend.at[k], rrecv.at[k], to))
        s = sign * parity(to_x, to_y)
        what = block(near(s * (a - to_x), s * (b - to_y)))
        t_second_from.append(remote(what, what, rsend.at[k], rrecv.at[k], to))

    def holder(q, d):
        ax, ay = HOLD[q]
        dx, dy = served(q)[d]
        s = sign * parity(ax + dx, ay + dy)
        return near(-s * dx, -s * dy), near(-s * (ax + dx), -s * (ay + dy))

    l_copies, ins = {}, {}
    for q in range(4):
        for d in (1, 2, 3):
            h, j = holder(q, d)
            l_copies[q, d] = remote(
                amps.at[:, j], lbuf.at[q, :, d], lsend.at[q, d - 1], lrecv.at[q, d - 1], h
            )
            ins[q, d] = remote(
                done.at[q, d - 1], out.at[0, j], osend.at[q, d - 1], orecv.at[q, d - 1], h
            )

    b_copies = {}
    for p, q, (dx, dy), chunks in EDGES:
        s = sign * parity(*HOLD[p])
        for c in chunks:
            piece = pl.ds(*PIECES[c])
            b_copies[q, c] = remote(
                bbuf[p].at[piece], bbuf[q].at[piece],
                bsend.at[q - 1, c], brecv.at[q - 1, c], near(s * dx, s * dy),
            )

    gives = {}
    for q in range(4):
        for d in range(4):
            gives[q, d] = partner(
                give.at[q, d], take.at[q, d], psend.at[q, d], precv.at[q, d]
            )

    outs = {}
    for q in range(4):
        s = sign * parity(*HOLD[q])
        for d in (1, 2, 3):
            dx, dy = served(q)[d]
            outs[q, d] = remote(
                done.at[q, d - 1], out.at[0, held(q)],
                osend.at[q, d - 1], orecv.at[q, d - 1], near(s * dx, s * dy),
            )

    mask_load.wait()
    nxt[32] = 31

    def search(k, c):
        p = 31 - k
        live = mask[lax.shift_right_logical(p, 3), lax.bitwise_and(p, 7), vir]
        c = live * p + (1 - live) * c
        nxt[p] = c
        return c

    lax.fori_loop(0, 32, search, 31)

    for copy in loads:
        copy.wait()

    def pack(k, p):
        p = nxt[p]
        bbuf0[k + lax.shift_right_logical(k, 2)] = xbuf[
            lax.bitwise_and(p, 7), lax.shift_right_logical(p, 3)
        ]
        return p + 1

    lax.fori_loop(0, 16, pack, 0)

    def dress(q):
        j = held(q)

        def columns(n, carry):
            amount = jnp.concatenate([bbuf[q][CHUNK * e + 4] for e in range(4)], axis=0)
            inner = lax.dot_general(
                amount,
                tbuf[pl.ds(2 * n, 2)].reshape(2 * TILE, TILE),
                (((1,), (1,)), ((), ())),
                preferred_element_type=jnp.float32,
            )
            for e in range(4):
                for k in range(2):
                    gate = mask[e, 2 * n + k, j].astype(jnp.float32)
                    value = bbuf[q][slot[q, 8 * e + 2 * n + k]].astype(jnp.float32)
                    value -= inner[e * TILE : (e + 1) * TILE, k * TILE : (k + 1) * TILE]
                    dense[q, n, e * TILE : (e + 1) * TILE, k * TILE : (k + 1) * TILE] = (
                        gate * value
                    ).astype(jnp.bfloat16)
            return carry

        lax.fori_loop(0, 4, columns, 0)

    def multiply(q, d):
        if d:
            l_copies[q, d].wait_recv()
        else:
            own_l[q].wait()
        lhs = jnp.concatenate([lbuf[q, other, d], lbuf[q, ka, d]], axis=0)
        for n in range(4):
            where = pl.ds(n * 2 * TILE, 2 * TILE)
            part = jnp.dot(lhs, dense[q, n], preferred_element_type=jnp.float32)
            give[q, d, :, where] = part[:64].astype(jnp.bfloat16)
            acc[q, d, :, where] = part[64:]
        gives[q, d].start()

    def finish(q, d):
        gives[q, d].wait_recv()
        total = acc[q, d] + take[q, d].astype(jnp.float32)
        if d:
            done[q, d - 1] = total.astype(jnp.bfloat16)
            outs[q, d].start()
        else:
            out[0, held(q)] = total.astype(jnp.bfloat16)

    def tables():
        for q in range(4):
            j = held(q)

            def count(p, c, q=q, j=j):
                live = mask[lax.shift_right_logical(p, 3), lax.bitwise_and(p, 7), j]
                slot[q, p] = live * (c + lax.shift_right_logical(c, 2)) + (1 - live) * EMPTY
                return c + live

            lax.fori_loop(0, 32, count, 0)
            bbuf[q][EMPTY] = jnp.zeros((TILE, TILE), jnp.bfloat16)

    def units(*which):
        for k, unit in enumerate(which):
            multiply(*unit)
            if k >= LAG:
                finish(*which[k - LAG])
        for unit in which[-LAG:]:
            finish(*unit)

    def rows(*which):
        for q, d in which:
            l_copies[q, d].start()

    def blocks(q, *which):
        for c in which:
            b_copies[q, c].start()

    def arrived(q, *which):
        for c in which:
            b_copies[q, c].wait_recv()

    t_half = partner(tbuf.at[:, :, ka], tbuf.at[:, :, ka], dsend, drecv)
    t_other = partner(tbuf.at[:, :, other], tbuf.at[:, :, other], dsend, drecv)

    def t_on():
        for copy in t_from:
            copy.wait_recv()
        for copy in t_second:
            copy.start()

    def t_across():
        for copy in t_second_from:
            copy.wait_recv()
        t_half.start()

    def relay(q, c, r):
        b_copies[q, c].wait_recv()
        b_copies[r, c].start()

    own_t.wait()
    pl.semaphore_wait(barrier, 9)

    for copy in t_first:
        copy.start()
    blocks(1, 0, 1)
    blocks(2, 2, 3)
    rows((0, 1), (0, 2))
    blocks(1, 4, 5)
    blocks(2, 6, 7)
    blocks(1, 6, 7)
    blocks(2, 4, 5)
    rows((3, 1), (3, 2), (2, 1), (1, 2))
    tables()
    relay(1, 0, 3)
    relay(2, 2, 3)
    t_on()
    relay(1, 1, 3)
    relay(2, 3, 3)
    relay(1, 4, 3)
    relay(2, 6, 3)
    relay(3, 0, 2)
    relay(3, 2, 1)
    relay(1, 5, 3)
    relay(2, 7, 3)
    t_across()
    relay(3, 1, 2)
    relay(3, 3, 1)
    rows((1, 3), (1, 1), (2, 2), (0, 3), (3, 3), (2, 3))
    t_other.wait_recv()
    dress(0)
    multiply(0, 1)
    multiply(0, 2)
    multiply(0, 0)
    arrived(2, 0, 1, 4, 5)
    dress(2)
    finish(0, 1)
    finish(0, 2)
    arrived(3, 4, 5, 6, 7)
    dress(3)
    multiply(3, 1)
    multiply(3, 2)
    multiply(2, 1)
    multiply(2, 0)
    multiply(3, 0)
    finish(3, 1)
    finish(3, 2)
    arrived(1, 2, 3, 6, 7)
    dress(1)
    finish(2, 1)
    multiply(1, 3)
    multiply(1, 2)
    multiply(1, 1)
    multiply(1, 0)
    finish(1, 3)
    finish(1, 2)
    finish(1, 1)
    multiply(0, 3)
    multiply(2, 2)
    multiply(3, 3)
    finish(0, 3)
    multiply(2, 3)
    finish(2, 2)
    finish(3, 3)
    finish(2, 3)
    finish(0, 0)
    finish(1, 0)
    finish(2, 0)
    finish(3, 0)

    for copy in t_first + t_second + [t_half]:
        copy.wait_send()
    for copies in (l_copies, b_copies, outs, gives):
        for copy in copies.values():
            copy.wait_send()
    for copy in ins.values():
        copy.wait_recv()

def body(lambda_amps, screened_ints, half_ints, singles, block_mask):
    bf16, f32 = jnp.bfloat16, jnp.float32
    dma = pltpu.SemaphoreType.DMA
    anywhere = pl.BlockSpec(memory_space=pl.ANY)
    return pl.pallas_call(
        kernel,
        out_shape=pltpu.VMEM((1, 16, 64, 1024), bf16),
        in_specs=[anywhere] * 5,
        out_specs=pl.BlockSpec(memory_space=pltpu.VMEM),
        scratch_shapes=[
            pltpu.VMEM((4, 2, 4, 64, 512), bf16),
            pltpu.VMEM((EMPTY + 1, TILE, TILE), bf16),
            pltpu.VMEM((EMPTY + 1, TILE, TILE), bf16),
            pltpu.VMEM((EMPTY + 1, TILE, TILE), bf16),
            pltpu.VMEM((EMPTY + 1, TILE, TILE), bf16),
            pltpu.VMEM((8, 4, TILE, TILE), bf16),
            pltpu.VMEM((8, 2, 2, 32, TILE), bf16),
            pltpu.VMEM((4, 4, 512, 2 * TILE), bf16),
            pltpu.VMEM((4, 4, 64, 1024), bf16),
            pltpu.VMEM((4, 4, 64, 1024), bf16),
            pltpu.VMEM((4, 4, 64, 1024), f32),
            pltpu.VMEM((4, 3, 64, 1024), bf16),
            pltpu.SMEM((4, 8, 16), jnp.int32),
            pltpu.SMEM((4, 32), jnp.int32),
            pltpu.SMEM((40,), jnp.int32),
            dma((4, 3)), dma((4, 3)), dma((4,)), dma((38,)),
            dma((8,)), dma((8,)), dma((7,)), dma((7,)), dma, dma,
            dma((3, 8)), dma((3, 8)),
            dma((4, 4)), dma((4, 4)), dma((4, 3)), dma((4, 3)),
        ],
        compiler_params=pltpu.CompilerParams(collective_id=0, has_side_effects=True),
        cost_estimate=pl.CostEstimate(
            flops=2 * 2048 * 512 * 1024, bytes_accessed=6 << 20, transcendentals=0
        ),
    )(
        lambda_amps, screened_ints, half_ints, singles.T,
        jnp.transpose(block_mask, (1, 2, 0)),
    )


def solution(mesh):
    return jax.shard_map(
        body,
        mesh=mesh,
        in_specs=(
            P(None, "occ", "vir", "ka"),
            P(("occ", "vir"), "ka", None),
            P(("occ", "vir"), "ka", None),
            P(None, "vir"),
            P("occ", "ka", None),
        ),
        out_specs=P("ka", "occ", "vir", None),
        check_vma=False,
    )
```

```python
import jax
import jax.numpy as jnp
from jax import lax
from jax.experimental import pallas as pl
from jax.experimental.pallas import tpu as pltpu
from jax.sharding import PartitionSpec as P

MESH = pl.DeviceIdType.MESH
TILE = 128
CHUNK = 5
EMPTY = 20
LAG = 5
SIDE = 4
HOLD = ((0, 0), (1, 0), (0, 1), (1, 1))
AROUND = tuple((a, b) for a in (-1, 0, 1) for b in (-1, 0, 1) if (a, b) != (0, 0))
EDGES = (
    (0, 1, (1, 0), (0, 1, 4, 5, 6, 7)),
    (0, 2, (0, 1), (2, 3, 4, 5, 6, 7)),
    (1, 3, (0, 1), (0, 1, 4, 5)),
    (2, 3, (1, 0), (2, 3, 6, 7)),
    (3, 2, (-1, 0), (0, 1)),
    (3, 1, (0, -1), (2, 3)),
)
PIECES = tuple((CHUNK * (c // 2) + 3 * (c % 2), 3 - c % 2) for c in range(8))
RELAYS = (
    ((1, -1), (-1, 0)), ((1, 0), (-1, 0)), ((1, 1), (-1, 0)),
    ((-1, 1), (0, -1)), ((0, 1), (0, -1)), ((1, 1), (0, -1)),
    ((1, 1), (-1, -1)),
)


def served(q):
    ax, ay = HOLD[q]
    ux, uy = 2 * ax - 1, 2 * ay - 1
    return ((0, 0), (ux, 0), (0, uy), (ux, uy))


def parity(a, b):
    return 1 - 2 * ((a + b) % 2)


def wrap(k):
    return lax.rem(k + 2 * SIDE, SIDE)


def place(x, y):
    return wrap(y) * SIDE + wrap(x)


def kernel(
    amps, ints, half, singles, mask_in, out,
    lbuf, bbuf0, bbuf1, bbuf2, bbuf3, xbuf, tbuf, dense, give, take, acc, done,
    mask, slot, nxt,
    lsend, lrecv, lown, inload, tsend, trecv, rsend, rrecv, dsend, drecv, bsend, brecv,
    psend, precv, osend, orecv,
):
    bbuf = (bbuf0, bbuf1, bbuf2, bbuf3)
    vir = lax.axis_index("vir")
    ka = lax.axis_index("ka")
    other = 1 - ka
    x, y = lax.rem(vir, SIDE), vir // SIDE
    sign = 1 - 2 * lax.rem(x + y, 2)

    def near(a, b):
        return place(x + a, y + b)

    def block(v):
        return tbuf.at[v // 2, lax.rem(v, 2), ka]

    def held(q):
        ax, ay = HOLD[q]
        s = sign * parity(ax, ay)
        return near(-s * ax, -s * ay)

    def remote(src, dst, send, recv, v):
        return pltpu.make_async_remote_copy(
            src_ref=src, dst_ref=dst, send_sem=send, recv_sem=recv,
            device_id={"vir": v}, device_id_type=MESH,
        )

    def partner(src, dst, send, recv):
        return pltpu.make_async_remote_copy(
            src_ref=src, dst_ref=dst, send_sem=send, recv_sem=recv,
            device_id={"ka": other}, device_id_type=MESH,
        )

    barrier = pltpu.get_barrier_semaphore()
    for a, b in AROUND:
        pl.semaphore_signal(
            barrier, inc=1, device_id={"vir": near(a, b)}, device_id_type=MESH
        )
    pl.semaphore_signal(barrier, inc=1, device_id={"ka": other}, device_id_type=MESH)

    own_t = pltpu.make_async_copy(singles.at[pl.ds(ka * 32, 32)], block(vir), inload.at[0])
    own_t.start()
    mask_load = pltpu.make_async_copy(mask_in, mask, inload.at[1])
    mask_load.start()
    loads = [
        pltpu.make_async_copy(half.at[0, pl.ds(e * TILE, TILE)], bbuf0.at[CHUNK * e + 4], inload.at[2 + e])
        for e in range(4)
    ]
    loads += [
        pltpu.make_async_copy(
            ints.at[0, pl.ds(e * TILE, TILE), pl.ds(b * TILE, TILE)],
            xbuf.at[b, e],
            inload.at[6 + 4 * b + e],
        )
        for b in range(8)
        for e in range(4)
    ]
    loads += [
        pltpu.make_async_copy(amps.at[:, held(q)], lbuf.at[q, :, 0], lown.at[q])
        for q in range(4)
    ]
    for copy in loads:
        copy.start()
    own_l = loads[-4:]
    loads = loads[:-4]

    t_first = [
        remote(block(vir), block(vir), tsend.at[k], trecv.at[k], near(a, b))
        for k, (a, b) in enumerate(AROUND)
    ]
    t_from = [
        remote(block(near(-a, -b)), block(near(-a, -b)), tsend.at[k], trecv.at[k], near(a, b))
        for k, (a, b) in enumerate(AROUND)
    ]
    t_second, t_second_from = [], []
    for k, ((a, b), (to_x, to_y)) in enumerate(RELAYS):
        what = block(near(sign * a, sign * b))
        to = near(sign * to_x, sign * to_y)
        t_second.append(remote(what, what, rsend.at[k], rrecv.at[k], to))
        s = sign * parity(to_x, to_y)
        what = block(near(s * (a - to_x), s * (b - to_y)))
        t_second_from.append(remote(what, what, rsend.at[k], rrecv.at[k], to))

    def holder(q, d):
        ax, ay = HOLD[q]
        dx, dy = served(q)[d]
        s = sign * parity(ax + dx, ay + dy)
        return near(-s * dx, -s * dy), near(-s * (ax + dx), -s * (ay + dy))

    l_copies, ins = {}, {}
    for q in range(4):
        for d in (1, 2, 3):
            h, j = holder(q, d)
            l_copies[q, d] = remote(
                amps.at[:, j], lbuf.at[q, :, d], lsend.at[q, d - 1], lrecv.at[q, d - 1], h
            )
            ins[q, d] = remote(
                done.at[q, d - 1], out.at[0, j], osend.at[q, d - 1], orecv.at[q, d - 1], h
            )

    b_copies = {}
    for p, q, (dx, dy), chunks in EDGES:
        s = sign * parity(*HOLD[p])
        for c in chunks:
            piece = pl.ds(*PIECES[c])
            b_copies[q, c] = remote(
                bbuf[p].at[piece], bbuf[q].at[piece],
                bsend.at[q - 1, c], brecv.at[q - 1, c], near(s * dx, s * dy),
            )

    gives = {}
    for q in range(4):
        for d in range(4):
            gives[q, d] = partner(
                give.at[q, d], take.at[q, d], psend.at[q, d], precv.at[q, d]
            )

    outs = {}
    for q in range(4):
        s = sign * parity(*HOLD[q])
        for d in (1, 2, 3):
            dx, dy = served(q)[d]
            outs[q, d] = remote(
                done.at[q, d - 1], out.at[0, held(q)],
                osend.at[q, d - 1], orecv.at[q, d - 1], near(s * dx, s * dy),
            )

    mask_load.wait()
    nxt[32] = 31

    def search(k, c):
        p = 31 - k
        live = mask[lax.shift_right_logical(p, 3), lax.bitwise_and(p, 7), vir]
        c = live * p + (1 - live) * c
        nxt[p] = c
        return c

    lax.fori_loop(0, 32, search, 31)

    for copy in loads:
        copy.wait()

    def pack(k, p):
        p = nxt[p]
        bbuf0[k + lax.shift_right_logical(k, 2)] = xbuf[
            lax.bitwise_and(p, 7), lax.shift_right_logical(p, 3)
        ]
        return p + 1

    lax.fori_loop(0, 16, pack, 0)

    def dress(q):
        j = held(q)

        def columns(n, carry):
            amount = jnp.concatenate([bbuf[q][CHUNK * e + 4] for e in range(4)], axis=0)
            inner = lax.dot_general(
                amount,
                tbuf[pl.ds(2 * n, 2)].reshape(2 * TILE, TILE),
                (((1,), (1,)), ((), ())),
                preferred_element_type=jnp.float32,
            )
            for e in range(4):
                for k in range(2):
                    gate = mask[e, 2 * n + k, j].astype(jnp.float32)
                    value = bbuf[q][slot[q, 8 * e + 2 * n + k]].astype(jnp.float32)
                    value -= inner[e * TILE : (e + 1) * TILE, k * TILE : (k + 1) * TILE]
                    dense[q, n, e * TILE : (e + 1) * TILE, k * TILE : (k + 1) * TILE] = (
                        gate * value
                    ).astype(jnp.bfloat16)
            return carry

        lax.fori_loop(0, 4, columns, 0)

    def multiply(q, d):
        if d:
            l_copies[q, d].wait_recv()
        else:
            own_l[q].wait()
        lhs = jnp.concatenate([lbuf[q, other, d], lbuf[q, ka, d]], axis=0)
        for n in range(4):
            where = pl.ds(n * 2 * TILE, 2 * TILE)
            part = jnp.dot(lhs, dense[q, n], preferred_element_type=jnp.float32)
            give[q, d, :, where] = part[:64].astype(jnp.bfloat16)
            acc[q, d, :, where] = part[64:]
        gives[q, d].start()

    def finish(q, d):
        gives[q, d].wait_recv()
        total = acc[q, d] + take[q, d].astype(jnp.float32)
        if d:
            done[q, d - 1] = total.astype(jnp.bfloat16)
            outs[q, d].start()
        else:
            out[0, held(q)] = total.astype(jnp.bfloat16)

    def tables():
        for q in range(4):
            j = held(q)

            def count(p, c, q=q, j=j):
                live = mask[lax.shift_right_logical(p, 3), lax.bitwise_and(p, 7), j]
                slot[q, p] = live * (c + lax.shift_right_logical(c, 2)) + (1 - live) * EMPTY
                return c + live

            lax.fori_loop(0, 32, count, 0)
            bbuf[q][EMPTY] = jnp.zeros((TILE, TILE), jnp.bfloat16)

    def units(*which):
        for k, unit in enumerate(which):
            multiply(*unit)
            if k >= LAG:
                finish(*which[k - LAG])
        for unit in which[-LAG:]:
            finish(*unit)

    def rows(*which):
        for q, d in which:
            l_copies[q, d].start()

    def blocks(q, *which):
        for c in which:
            b_copies[q, c].start()

    def arrived(q, *which):
        for c in which:
            b_copies[q, c].wait_recv()

    t_half = partner(tbuf.at[:, :, ka], tbuf.at[:, :, ka], dsend, drecv)
    t_other = partner(tbuf.at[:, :, other], tbuf.at[:, :, other], dsend, drecv)

    def t_on():
        for copy in t_from:
            copy.wait_recv()
        for copy in t_second:
            copy.start()

    def t_across():
        for copy in t_second_from:
            copy.wait_recv()
        t_half.start()

    def relay(q, c, r):
        b_copies[q, c].wait_recv()
        b_copies[r, c].start()

    own_t.wait()
    pl.semaphore_wait(barrier, 9)

    for copy in t_first:
        copy.start()
    blocks(1, 0, 1)
    blocks(2, 2, 3)
    rows((0, 1), (0, 2))
    blocks(1, 4, 5)
    blocks(2, 6, 7)
    blocks(1, 6, 7)
    blocks(2, 4, 5)
    rows((3, 1), (3, 2), (2, 1), (1, 2))
    tables()
    relay(1, 0, 3)
    relay(2, 2, 3)
    t_on()
    relay(1, 1, 3)
    relay(2, 3, 3)
    relay(1, 4, 3)
    relay(2, 6, 3)
    relay(3, 0, 2)
    relay(3, 2, 1)
    relay(1, 5, 3)
    relay(2, 7, 3)
    t_across()
    relay(3, 1, 2)
    relay(3, 3, 1)
    rows((1, 3), (1, 1), (2, 2), (0, 3), (3, 3), (2, 3))
    t_other.wait_recv()
    dress(0)
    multiply(0, 1)
    multiply(0, 2)
    multiply(0, 0)
    finish(0, 1)
    finish(0, 2)
    arrived(2, 0, 1, 4, 5)
    dress(2)
    arrived(3, 4, 5, 6, 7)
    dress(3)
    multiply(3, 1)
    multiply(3, 2)
    multiply(2, 1)
    multiply(2, 0)
    multiply(3, 0)
    finish(3, 1)
    finish(3, 2)
    arrived(1, 2, 3, 6, 7)
    dress(1)
    finish(2, 1)
    multiply(1, 3)
    multiply(1, 2)
    multiply(1, 1)
    multiply(1, 0)
    finish(1, 3)
    finish(1, 2)
    finish(1, 1)
    multiply(0, 3)
    multiply(2, 2)
    multiply(3, 3)
    finish(0, 3)
    multiply(2, 3)
    finish(2, 2)
    finish(3, 3)
    finish(2, 3)
    finish(0, 0)
    finish(1, 0)
    finish(2, 0)
    finish(3, 0)

    for copy in t_first + t_second + [t_half]:
        copy.wait_send()
    for copies in (l_copies, b_copies, outs, gives):
        for copy in copies.values():
            copy.wait_send()
    for copy in ins.values():
        copy.wait_recv()

def body(lambda_amps, screened_ints, half_ints, singles, block_mask):
    bf16, f32 = jnp.bfloat16, jnp.float32
    dma = pltpu.SemaphoreType.DMA
    anywhere = pl.BlockSpec(memory_space=pl.ANY)
    return pl.pallas_call(
        kernel,
        out_shape=pltpu.VMEM((1, 16, 64, 1024), bf16),
        in_specs=[anywhere] * 5,
        out_specs=pl.BlockSpec(memory_space=pltpu.VMEM),
        scratch_shapes=[
            pltpu.VMEM((4, 2, 4, 64, 512), bf16),
            pltpu.VMEM((EMPTY + 1, TILE, TILE), bf16),
            pltpu.VMEM((EMPTY + 1, TILE, TILE), bf16),
            pltpu.VMEM((EMPTY + 1, TILE, TILE), bf16),
            pltpu.VMEM((EMPTY + 1, TILE, TILE), bf16),
            pltpu.VMEM((8, 4, TILE, TILE), bf16),
            pltpu.VMEM((8, 2, 2, 32, TILE), bf16),
            pltpu.VMEM((4, 4, 512, 2 * TILE), bf16),
            pltpu.VMEM((4, 4, 64, 1024), bf16),
            pltpu.VMEM((4, 4, 64, 1024), bf16),
            pltpu.VMEM((4, 4, 64, 1024), f32),
            pltpu.VMEM((4, 3, 64, 1024), bf16),
            pltpu.SMEM((4, 8, 16), jnp.int32),
            pltpu.SMEM((4, 32), jnp.int32),
            pltpu.SMEM((40,), jnp.int32),
            dma((4, 3)), dma((4, 3)), dma((4,)), dma((38,)),
            dma((8,)), dma((8,)), dma((7,)), dma((7,)), dma, dma,
            dma((3, 8)), dma((3, 8)),
            dma((4, 4)), dma((4, 4)), dma((4, 3)), dma((4, 3)),
        ],
        compiler_params=pltpu.CompilerParams(collective_id=0, has_side_effects=True),
        cost_estimate=pl.CostEstimate(
            flops=2 * 2048 * 512 * 1024, bytes_accessed=6 << 20, transcendentals=0
        ),
    )(
        lambda_amps, screened_ints, half_ints, singles.T,
        jnp.transpose(block_mask, (1, 2, 0)),
    )


def solution(mesh):
    return jax.shard_map(
        body,
        mesh=mesh,
        in_specs=(
            P(None, "occ", "vir", "ka"),
            P(("occ", "vir"), "ka", None),
            P(("occ", "vir"), "ka", None),
            P(None, "vir"),
            P("occ", "ka", None),
        ),
        out_specs=P("ka", "occ", "vir", None),
        check_vma=False,
    )
```

```python
import jax
import jax.numpy as jnp
from jax import lax
from jax.experimental import pallas as pl
from jax.experimental.pallas import tpu as pltpu
from jax.sharding import PartitionSpec as P

MESH = pl.DeviceIdType.MESH
TILE = 128
CHUNK = 5
EMPTY = 20
LAG = 5
SIDE = 4
HOLD = ((0, 0), (1, 0), (0, 1), (1, 1))
AROUND = tuple((a, b) for a in (-1, 0, 1) for b in (-1, 0, 1) if (a, b) != (0, 0))
EDGES = (
    (0, 1, (1, 0), (0, 1, 4, 5, 6, 7)),
    (0, 2, (0, 1), (2, 3, 4, 5, 6, 7)),
    (1, 3, (0, 1), (0, 1, 4, 5)),
    (2, 3, (1, 0), (2, 3, 6, 7)),
    (3, 2, (-1, 0), (0, 1)),
    (3, 1, (0, -1), (2, 3)),
)
PIECES = tuple((CHUNK * (c // 2) + 3 * (c % 2), 3 - c % 2) for c in range(8))
RELAYS = (
    ((1, -1), (-1, 0)), ((1, 0), (-1, 0)), ((1, 1), (-1, 0)),
    ((-1, 1), (0, -1)), ((0, 1), (0, -1)), ((1, 1), (0, -1)),
    ((1, 1), (-1, -1)),
)


def served(q):
    ax, ay = HOLD[q]
    ux, uy = 2 * ax - 1, 2 * ay - 1
    return ((0, 0), (ux, 0), (0, uy), (ux, uy))


def parity(a, b):
    return 1 - 2 * ((a + b) % 2)


def wrap(k):
    return lax.rem(k + 2 * SIDE, SIDE)


def place(x, y):
    return wrap(y) * SIDE + wrap(x)


def kernel(
    amps, ints, half, singles, mask_in, out,
    lbuf, bbuf0, bbuf1, bbuf2, bbuf3, xbuf, tbuf, dense, give, take, acc, done,
    mask, slot, nxt,
    lsend, lrecv, lown, inload, tsend, trecv, rsend, rrecv, dsend, drecv, bsend, brecv,
    psend, precv, osend, orecv,
):
    bbuf = (bbuf0, bbuf1, bbuf2, bbuf3)
    vir = lax.axis_index("vir")
    ka = lax.axis_index("ka")
    other = 1 - ka
    x, y = lax.rem(vir, SIDE), vir // SIDE
    sign = 1 - 2 * lax.rem(x + y, 2)

    def near(a, b):
        return place(x + a, y + b)

    def block(v):
        return tbuf.at[v // 2, lax.rem(v, 2), ka]

    def held(q):
        ax, ay = HOLD[q]
        s = sign * parity(ax, ay)
        return near(-s * ax, -s * ay)

    def remote(src, dst, send, recv, v):
        return pltpu.make_async_remote_copy(
            src_ref=src, dst_ref=dst, send_sem=send, recv_sem=recv,
            device_id={"vir": v}, device_id_type=MESH,
        )

    def partner(src, dst, send, recv):
        return pltpu.make_async_remote_copy(
            src_ref=src, dst_ref=dst, send_sem=send, recv_sem=recv,
            device_id={"ka": other}, device_id_type=MESH,
        )

    barrier = pltpu.get_barrier_semaphore()
    for a, b in AROUND:
        pl.semaphore_signal(
            barrier, inc=1, device_id={"vir": near(a, b)}, device_id_type=MESH
        )
    pl.semaphore_signal(barrier, inc=1, device_id={"ka": other}, device_id_type=MESH)

    own_t = pltpu.make_async_copy(singles.at[pl.ds(ka * 32, 32)], block(vir), inload.at[0])
    own_t.start()
    mask_load = pltpu.make_async_copy(mask_in, mask, inload.at[1])
    mask_load.start()
    loads = [
        pltpu.make_async_copy(half.at[0, pl.ds(e * TILE, TILE)], bbuf0.at[CHUNK * e + 4], inload.at[2 + e])
        for e in range(4)
    ]
    loads += [
        pltpu.make_async_copy(
            ints.at[0, pl.ds(e * TILE, TILE), pl.ds(b * TILE, TILE)],
            xbuf.at[b, e],
            inload.at[6 + 4 * b + e],
        )
        for b in range(8)
        for e in range(4)
    ]
    loads += [
        pltpu.make_async_copy(amps.at[:, held(q)], lbuf.at[q, :, 0], lown.at[q])
        for q in range(4)
    ]
    for copy in loads:
        copy.start()
    own_l = loads[-4:]
    loads = loads[:-4]

    t_first = [
        remote(block(vir), block(vir), tsend.at[k], trecv.at[k], near(a, b))
        for k, (a, b) in enumerate(AROUND)
    ]
    t_from = [
        remote(block(near(-a, -b)), block(near(-a, -b)), tsend.at[k], trecv.at[k], near(a, b))
        for k, (a, b) in enumerate(AROUND)
    ]
    t_second, t_second_from = [], []
    for k, ((a, b), (to_x, to_y)) in enumerate(RELAYS):
        what = block(near(sign * a, sign * b))
        to = near(sign * to_x, sign * to_y)
        t_second.append(remote(what, what, rsend.at[k], rrecv.at[k], to))
        s = sign * parity(to_x, to_y)
        what = block(near(s * (a - to_x), s * (b - to_y)))
        t_second_from.append(remote(what, what, rsend.at[k], rrecv.at[k], to))

    def holder(q, d):
        ax, ay = HOLD[q]
        dx, dy = served(q)[d]
        s = sign * parity(ax + dx, ay + dy)
        return near(-s * dx, -s * dy), near(-s * (ax + dx), -s * (ay + dy))

    l_copies, ins = {}, {}
    for q in range(4):
        for d in (1, 2, 3):
            h, j = holder(q, d)
            l_copies[q, d] = remote(
                amps.at[:, j], lbuf.at[q, :, d], lsend.at[q, d - 1], lrecv.at[q, d - 1], h
            )
            ins[q, d] = remote(
                done.at[q, d - 1], out.at[0, j], osend.at[q, d - 1], orecv.at[q, d - 1], h
            )

    b_copies = {}
    for p, q, (dx, dy), chunks in EDGES:
        s = sign * parity(*HOLD[p])
        for c in chunks:
            piece = pl.ds(*PIECES[c])
            b_copies[q, c] = remote(
                bbuf[p].at[piece], bbuf[q].at[piece],
                bsend.at[q - 1, c], brecv.at[q - 1, c], near(s * dx, s * dy),
            )

    gives = {}
    for q in range(4):
        for d in range(4):
            gives[q, d] = partner(
                give.at[q, d], take.at[q, d], psend.at[q, d], precv.at[q, d]
            )

    outs = {}
    for q in range(4):
        s = sign * parity(*HOLD[q])
        for d in (1, 2, 3):
            dx, dy = served(q)[d]
            outs[q, d] = remote(
                done.at[q, d - 1], out.at[0, held(q)],
                osend.at[q, d - 1], orecv.at[q, d - 1], near(s * dx, s * dy),
            )

    mask_load.wait()
    nxt[32] = 31

    def search(k, c):
        p = 31 - k
        live = mask[lax.shift_right_logical(p, 3), lax.bitwise_and(p, 7), vir]
        c = live * p + (1 - live) * c
        nxt[p] = c
        return c

    lax.fori_loop(0, 32, search, 31)

    for copy in loads:
        copy.wait()

    def pack(k, p):
        p = nxt[p]
        bbuf0[k + lax.shift_right_logical(k, 2)] = xbuf[
            lax.bitwise_and(p, 7), lax.shift_right_logical(p, 3)
        ]
        return p + 1

    lax.fori_loop(0, 16, pack, 0)

    def dress(q):
        j = held(q)

        def columns(n, carry):
            amount = jnp.concatenate([bbuf[q][CHUNK * e + 4] for e in range(4)], axis=0)
            inner = lax.dot_general(
                amount,
                tbuf[pl.ds(2 * n, 2)].reshape(2 * TILE, TILE),
                (((1,), (1,)), ((), ())),
                preferred_element_type=jnp.float32,
            )
            for e in range(4):
                for k in range(2):
                    gate = mask[e, 2 * n + k, j].astype(jnp.float32)
                    value = bbuf[q][slot[q, 8 * e + 2 * n + k]].astype(jnp.float32)
                    value -= inner[e * TILE : (e + 1) * TILE, k * TILE : (k + 1) * TILE]
                    dense[q, n, e * TILE : (e + 1) * TILE, k * TILE : (k + 1) * TILE] = (
                        gate * value
                    ).astype(jnp.bfloat16)
            return carry

        lax.fori_loop(0, 4, columns, 0)

    def multiply(q, d):
        if d:
            l_copies[q, d].wait_recv()
        else:
            own_l[q].wait()
        lhs = jnp.concatenate([lbuf[q, other, d], lbuf[q, ka, d]], axis=0)
        for n in range(4):
            where = pl.ds(n * 2 * TILE, 2 * TILE)
            part = jnp.dot(lhs, dense[q, n], preferred_element_type=jnp.float32)
            give[q, d, :, where] = part[:64].astype(jnp.bfloat16)
            acc[q, d, :, where] = part[64:]
        gives[q, d].start()

    def finish(q, d):
        gives[q, d].wait_recv()
        total = acc[q, d] + take[q, d].astype(jnp.float32)
        if d:
            done[q, d - 1] = total.astype(jnp.bfloat16)
            outs[q, d].start()
        else:
            out[0, held(q)] = total.astype(jnp.bfloat16)

    def tables():
        for q in range(4):
            j = held(q)

            def count(p, c, q=q, j=j):
                live = mask[lax.shift_right_logical(p, 3), lax.bitwise_and(p, 7), j]
                slot[q, p] = live * (c + lax.shift_right_logical(c, 2)) + (1 - live) * EMPTY
                return c + live

            lax.fori_loop(0, 32, count, 0)
            bbuf[q][EMPTY] = jnp.zeros((TILE, TILE), jnp.bfloat16)

    def units(*which):
        for k, unit in enumerate(which):
            multiply(*unit)
            if k >= LAG:
                finish(*which[k - LAG])
        for unit in which[-LAG:]:
            finish(*unit)

    def rows(*which):
        for q, d in which:
            l_copies[q, d].start()

    def blocks(q, *which):
        for c in which:
            b_copies[q, c].start()

    def arrived(q, *which):
        for c in which:
            b_copies[q, c].wait_recv()

    t_half = partner(tbuf.at[:, :, ka], tbuf.at[:, :, ka], dsend, drecv)
    t_other = partner(tbuf.at[:, :, other], tbuf.at[:, :, other], dsend, drecv)

    def t_on():
        for copy in t_from:
            copy.wait_recv()
        for copy in t_second:
            copy.start()

    def t_across():
        for copy in t_second_from:
            copy.wait_recv()
        t_half.start()

    def relay(q, c, r):
        b_copies[q, c].wait_recv()
        b_copies[r, c].start()

    own_t.wait()
    pl.semaphore_wait(barrier, 9)

    for copy in t_first:
        copy.start()
    blocks(1, 0, 1)
    blocks(2, 2, 3)
    rows((0, 1), (0, 2))
    blocks(1, 4, 5)
    blocks(2, 6, 7)
    blocks(1, 6, 7)
    blocks(2, 4, 5)
    rows((3, 1), (3, 2), (2, 1), (1, 2))
    tables()
    relay(1, 0, 3)
    relay(2, 2, 3)
    t_on()
    relay(1, 1, 3)
    relay(2, 3, 3)
    relay(1, 4, 3)
    relay(2, 6, 3)
    relay(3, 0, 2)
    relay(3, 2, 1)
    relay(1, 5, 3)
    relay(2, 7, 3)
    relay(3, 1, 2)
    relay(3, 3, 1)
    rows((1, 3), (1, 1), (2, 2), (0, 3), (3, 3), (2, 3))
    t_across()
    t_other.wait_recv()
    dress(0)
    multiply(0, 1)
    multiply(0, 2)
    multiply(0, 0)
    arrived(2, 0, 1, 4, 5)
    dress(2)
    finish(0, 1)
    finish(0, 2)
    arrived(3, 4, 5, 6, 7)
    dress(3)
    multiply(3, 1)
    multiply(3, 2)
    multiply(2, 1)
    multiply(2, 0)
    multiply(3, 0)
    finish(3, 1)
    finish(3, 2)
    arrived(1, 2, 3, 6, 7)
    dress(1)
    finish(2, 1)
    multiply(1, 3)
    multiply(1, 2)
    multiply(1, 1)
    multiply(1, 0)
    finish(1, 3)
    finish(1, 2)
    finish(1, 1)
    multiply(0, 3)
    multiply(2, 2)
    multiply(3, 3)
    finish(0, 3)
    multiply(2, 3)
    finish(2, 2)
    finish(3, 3)
    finish(2, 3)
    finish(0, 0)
    finish(1, 0)
    finish(2, 0)
    finish(3, 0)

    for copy in t_first + t_second + [t_half]:
        copy.wait_send()
    for copies in (l_copies, b_copies, outs, gives):
        for copy in copies.values():
            copy.wait_send()
    for copy in ins.values():
        copy.wait_recv()

def body(lambda_amps, screened_ints, half_ints, singles, block_mask):
    bf16, f32 = jnp.bfloat16, jnp.float32
    dma = pltpu.SemaphoreType.DMA
    anywhere = pl.BlockSpec(memory_space=pl.ANY)
    return pl.pallas_call(
        kernel,
        out_shape=pltpu.VMEM((1, 16, 64, 1024), bf16),
        in_specs=[anywhere] * 5,
        out_specs=pl.BlockSpec(memory_space=pltpu.VMEM),
        scratch_shapes=[
            pltpu.VMEM((4, 2, 4, 64, 512), bf16),
            pltpu.VMEM((EMPTY + 1, TILE, TILE), bf16),
            pltpu.VMEM((EMPTY + 1, TILE, TILE), bf16),
            pltpu.VMEM((EMPTY + 1, TILE, TILE), bf16),
            pltpu.VMEM((EMPTY + 1, TILE, TILE), bf16),
            pltpu.VMEM((8, 4, TILE, TILE), bf16),
            pltpu.VMEM((8, 2, 2, 32, TILE), bf16),
            pltpu.VMEM((4, 4, 512, 2 * TILE), bf16),
            pltpu.VMEM((4, 4, 64, 1024), bf16),
            pltpu.VMEM((4, 4, 64, 1024), bf16),
            pltpu.VMEM((4, 4, 64, 1024), f32),
            pltpu.VMEM((4, 3, 64, 1024), bf16),
            pltpu.SMEM((4, 8, 16), jnp.int32),
            pltpu.SMEM((4, 32), jnp.int32),
            pltpu.SMEM((40,), jnp.int32),
            dma((4, 3)), dma((4, 3)), dma((4,)), dma((38,)),
            dma((8,)), dma((8,)), dma((7,)), dma((7,)), dma, dma,
            dma((3, 8)), dma((3, 8)),
            dma((4, 4)), dma((4, 4)), dma((4, 3)), dma((4, 3)),
        ],
        compiler_params=pltpu.CompilerParams(collective_id=0, has_side_effects=True),
        cost_estimate=pl.CostEstimate(
            flops=2 * 2048 * 512 * 1024, bytes_accessed=6 << 20, transcendentals=0
        ),
    )(
        lambda_amps, screened_ints, half_ints, singles.T,
        jnp.transpose(block_mask, (1, 2, 0)),
    )


def solution(mesh):
    return jax.shard_map(
        body,
        mesh=mesh,
        in_specs=(
            P(None, "occ", "vir", "ka"),
            P(("occ", "vir"), "ka", None),
            P(("occ", "vir"), "ka", None),
            P(None, "vir"),
            P("occ", "ka", None),
        ),
        out_specs=P("ka", "occ", "vir", None),
        check_vma=False,
    )
```
